32 devices in a mesh: unit: 2 (over core), zero: 4 (over z), model: 4 (over y, x).
Axes of the slice: x: 2, y: 2, z: 4, core: 2. Of those that a mesh axis runs over, the one named last changes fastest.
Arguments:
- first_query: float32 [16384, 8192], P(('unit', 'zero'), 'model'), parts along dimension 0, may hold values from -0.09375 to 0.09375
- second_query: float32 [16384, 8192], P(('unit', 'zero'), 'model'), parts along dimension 0, may hold values from -0.0625 to 0.0625
- first_key: float32 [16384, 1024], P(('unit', 'zero'), 'model'), parts along dimension 0, may hold values from -0.09375 to 0.09375
- second_key: float32 [16384, 1024], P(('unit', 'zero'), 'model'), parts along dimension 0, may hold values from -0.0625 to 0.0625
- first_value: float32 [16384, 1024], P(('unit', 'zero'), 'model'), parts along dimension 0, may hold values from -0.09375 to 0.09375
- second_value: float32 [16384, 1024], P(('unit', 'zero'), 'model'), parts along dimension 0, may hold values from -0.0625 to 0.0625
- mix_share: float32 [16384], P(('unit', 'zero')), parts along dimension 0, may hold values from 0.2 to 0.8
- norm_train: float32 [16384], P(('unit', 'zero', 'model')), parts along dimension 0, may hold values from 0.25 to 1.75
- norm_step: float32 [16384], P(('unit', 'zero', 'model')), parts along dimension 0, may hold values from -0.3 to 0.3
Outputs:
- serve_query: bfloat16 [16384, 8192], P('unit', 'model'), parts along dimension 0
- serve_key: bfloat16 [16384, 1024], P('unit', 'model'), parts along dimension 0
- serve_value: bfloat16 [16384, 1024], P('unit', 'model'), parts along dimension 0
- factor_query: float32 [16384], P(('unit', 'model')), parts along dimension 0
- factor_key: float32 [2048], P(('unit', 'model')), parts along dimension 0
- factor_value: float32 [2048], P(('unit', 'model')), parts along dimension 0
- serve_norm: bfloat16 [16384], P('unit'), parts along dimension 0
The draws below stay inside these ranges and needn't reach their ends.
There are 2 independent parts, one for each index of `unit`. The reference program is written for one: setup_inputs(seed, part) draws one part's arguments, and reference() takes and returns one part's arrays. A program takes and returns all parts, laid end to end along the dimension named above; each array names one. Nothing has to cross between parts.
All inputs are finite; a program needn't handle non-finite values.
Results may differ from the reference program's by a relative error of at most 0.0004.
Values may be sent and summed in bfloat16 or wider, within the bound.
No kernel may reach another device: no remote copies, remote signals or barrier semaphores. Data moves between devices by JAX's collectives and lax.ppermute only.
A program may use at most 192 MiB of HBM per device.

```python
import jax
import jax.numpy as jnp
from jax import lax

D_MODEL = 8192
Q_DIM = 8192
KV_DIM = 1024


def with_spikes(values, rng, source, target, shards_of, factor):
    owner, partner = [(jnp.arange(values.shape[dim]) // (values.shape[dim] // shards_of)).reshape([-1 if axis == dim else 1 for axis in range(values.ndim)]) for dim in (source, target)]
    chosen = jax.random.permutation(rng, shards_of)[partner]
    strong = (owner == chosen) | (owner == (partner + shards_of // 2) % shards_of)
    return jnp.where(strong, factor * values, values)


def level_of(rng, shape, cuts, smallest, high):
    def one(axis_at, blocks):
        draws = jax.random.uniform(jax.random.fold_in(jax.random.fold_in(rng, 6), axis_at), (blocks,), jnp.float32, smallest / len(cuts), high / len(cuts))
        return jnp.repeat(jnp.exp(draws), shape[axis_at] // blocks).reshape((-1,) + (1,) * (len(shape) - axis_at - 1))

    loudness = one(*cuts[0])
    for cut in cuts[1:]:
        loudness = loudness * one(*cut)
    return loudness


def normal_values(stream_key, extent, deviation, reach, cuts=(), dtype=jnp.bfloat16):
    entries = deviation * jax.random.normal(stream_key, extent, jnp.float32)
    if cuts:
        entries = entries * level_of(stream_key, extent, cuts, -0.22, 0.18)
    return jnp.clip(entries, -reach, reach).astype(dtype)


def noise_with(own_key, extent, deviation, most, cuts, heavy, held_as=jnp.bfloat16):
    values = deviation * jax.random.normal(own_key, extent, jnp.float32)
    if cuts:
        values = values * level_of(own_key, extent, cuts, -0.22, 0.18)
    return jnp.clip(with_spikes(values, jax.random.fold_in(own_key, 3), *heavy), -most, most).astype(held_as)


def setup_inputs(seed: int = 0, part: int = 0) -> dict:
    key_list = jax.random.split(jax.random.key(seed), 10)
    own_keys = jax.random.split(jax.random.fold_in(key_list[9], part), 10)
    return {
        "first_query": noise_with(own_keys[0], (D_MODEL, Q_DIM), D_MODEL ** -0.5, 0.09375, ((0, 4), (1, 4)), (0, 1, 4, 2.0), jnp.float32),
        "second_query": normal_values(own_keys[1], (D_MODEL, Q_DIM), D_MODEL ** -0.5, 0.0625, ((0, 4), (1, 4)), jnp.float32),
        "first_key": noise_with(own_keys[2], (D_MODEL, KV_DIM), D_MODEL ** -0.5, 0.09375, ((0, 4), (1, 4)), (0, 1, 4, 2.0), jnp.float32),
        "second_key": normal_values(own_keys[3], (D_MODEL, KV_DIM), D_MODEL ** -0.5, 0.0625, ((0, 4), (1, 4)), jnp.float32),
        "first_value": noise_with(own_keys[4], (D_MODEL, KV_DIM), D_MODEL ** -0.5, 0.09375, ((0, 4), (1, 4)), (0, 1, 4, 2.0), jnp.float32),
        "second_value": normal_values(own_keys[5], (D_MODEL, KV_DIM), D_MODEL ** -0.5, 0.0625, ((0, 4), (1, 4)), jnp.float32),
        "mix_share": jnp.clip(0.2 + 0.6 * jax.random.uniform(own_keys[6], (D_MODEL,), jnp.float32) ** level_of(own_keys[6], (D_MODEL,), ((0, 4),), -0.2, 0.2), 0.2, 0.8),
        "norm_train": jnp.clip(1.0 + 0.15 * jax.random.normal(own_keys[7], (D_MODEL,), jnp.float32), 0.25, 1.75),
        "norm_step": jnp.clip(jax.random.uniform(own_keys[8], (D_MODEL,), jnp.float32, -0.3, 0.3) * level_of(own_keys[8], (D_MODEL,), ((0, 16),), -0.4, 0.0), -0.3, 0.3),
    }


def reference(first_query, second_query, first_key, second_key, first_value, second_value, mix_share, norm_train, norm_step):
    fresh_query = mix_share[:, None] * first_query + (1.0 - mix_share[:, None]) * second_query
    fresh_key = mix_share[:, None] * first_key + (1.0 - mix_share[:, None]) * second_key
    fresh_value = mix_share[:, None] * first_value + (1.0 - mix_share[:, None]) * second_value
    factor_query = jnp.sqrt(lax.optimization_barrier(jnp.sum(fresh_query * fresh_query, axis=0)))
    serve_query = (fresh_query / factor_query).astype(jnp.bfloat16)
    factor_key = jnp.sqrt(lax.optimization_barrier(jnp.sum(fresh_key * fresh_key, axis=0)))
    serve_key = (fresh_key / factor_key).astype(jnp.bfloat16)
    factor_value = jnp.sqrt(lax.optimization_barrier(jnp.sum(fresh_value * fresh_value, axis=0)))
    serve_value = (fresh_value / factor_value).astype(jnp.bfloat16)
    serve_norm = (norm_train + norm_step).astype(jnp.bfloat16)
    return (serve_query, serve_key, serve_value, factor_query, factor_key, factor_value, serve_norm)
```

```python
import functools

import jax
import jax.numpy as jnp
from jax import lax
from jax.experimental import pallas as pl
from jax.experimental.pallas import tpu as pltpu
from jax.sharding import PartitionSpec as P


PIECES = 8


def place_kernel(n, step, row, *refs):
    count = 3 if step == 1 else 2
    sources = refs[:count]
    out, buf, sem_in, sem_out = refs[count + 1 :]
    z = lax.axis_index("zero")
    rows = sources[0].shape[0]
    shard = out.shape[0] // n
    shards = [z + step, z - step, z]
    valid = [z + step < n, z >= step, None]

    def guarded(i, f):
        if valid[i] is None:
            f()
        else:
            pl.when(valid[i])(f)

    def take(i):
        return pltpu.make_async_copy(sources[i], buf.at[i], sem_in.at[i])

    def give(i):
        return pltpu.make_async_copy(
            buf.at[i], out.at[pl.ds(shards[i] * shard + row, rows)], sem_out.at[i]
        )

    for i in range(count):
        guarded(i, lambda i=i: take(i).start())
    for i in range(count):

        def pass_on(i=i):
            take(i).wait()
            give(i).start()

        guarded(i, pass_on)
    for i in range(count):
        guarded(i, lambda i=i: give(i).wait())


def place(n, step, row, out, *sources):
    rows, columns = sources[0].shape
    count = len(sources)
    any_spec = pl.BlockSpec(memory_space=pl.ANY)
    return pl.pallas_call(
        functools.partial(place_kernel, n, step, row),
        out_shape=jax.ShapeDtypeStruct(out.shape, out.dtype),
        in_specs=[any_spec] * (count + 1),
        out_specs=any_spec,
        input_output_aliases={count: 0},
        scratch_shapes=[
            pltpu.VMEM((count, rows, columns), out.dtype),
            pltpu.SemaphoreType.DMA((count,)),
            pltpu.SemaphoreType.DMA((count,)),
        ],
    )(*sources, out)


def blank_kernel(out):
    pass


def blank(shape, dtype):
    return pl.pallas_call(
        blank_kernel,
        out_shape=jax.ShapeDtypeStruct(shape, dtype),
        out_specs=pl.BlockSpec(memory_space=pl.ANY),
        name="blank",
    )()


def exchanged_sum(mine, n):
    if n > 4:
        return lax.psum(mine, "zero")
    z = lax.axis_index("zero")
    got = [mine]
    for k in range(1, n):
        got.append(lax.ppermute(mine, "zero", [(i, (i + k) % n) for i in range(n)]))
    ordered = [
        lax.select_n(lax.rem(z - i + n, n), *got) if n > 1 else mine for i in range(n)
    ]
    return sum(ordered[1:], ordered[0])


def on_device(
    n,
    first_query,
    second_query,
    first_key,
    second_key,
    first_value,
    second_value,
    mix_share,
    norm_train,
    norm_step,
):
    z = lax.axis_index("zero")
    share = mix_share[:, None]

    def squares(first, second):
        fresh = share * first + (1.0 - share) * second
        return jnp.sum(fresh * fresh, axis=0)

    def narrow(first, second, factor, row, rows):
        part = share[row : row + rows]
        fresh = part * first[row : row + rows] + (1.0 - part) * second[row : row + rows]
        return (fresh / factor).astype(jnp.bfloat16)

    wide = first_key.shape[1]
    rows = first_key.shape[0]
    mine_kv = jnp.concatenate((squares(first_key, second_key), squares(first_value, second_value)))
    factor_kv = jnp.sqrt(exchanged_sum(mine_kv, n))
    factor_key, factor_value = factor_kv[:wide], factor_kv[wide:]
    key = narrow(first_key, second_key, factor_key, 0, rows)
    first_value, second_value, key = lax.optimization_barrier((first_value, second_value, key))
    value = narrow(first_value, second_value, factor_value, 0, rows)

    mine_query = squares(first_query, second_query)
    factor_query = jnp.sqrt(exchanged_sum(mine_query, n))
    size = rows // PIECES
    queries = []
    for i in range(PIECES):
        queries.append(narrow(first_query, second_query, factor_query, i * size, size))
    norm = lax.all_gather((norm_train + norm_step).astype(jnp.bfloat16), "model", tiled=True)

    outs = [
        blank((n * rows, wide), jnp.bfloat16),
        blank((n * rows, wide), jnp.bfloat16),
        blank((n * rows, first_query.shape[1]), jnp.bfloat16),
    ]
    pieces = [(0, 0, key), (1, 0, value)] + [(2, i * size, q) for i, q in enumerate(queries)]
    lefts = [p for _, _, p in pieces]
    rights = [p for _, _, p in pieces]
    for j, step in sequence(n):
        which, row, own = pieces[j]
        lefts[j] = lax.ppermute(
            lefts[j], "zero", [(i, i - 1) for i in range(1, n - step + 1)]
        )
        rights[j] = lax.ppermute(rights[j], "zero", [(i, i + 1) for i in range(step - 1, n - 1)])
        sources = (lefts[j], rights[j]) + ((own,) if step == 1 else ())
        outs[which] = place(n, step, row, outs[which], *sources)
    full = jnp.zeros((n, norm.shape[0]), norm.dtype)
    full = lax.dynamic_update_index_in_dim(full, norm, z, 0)
    left = right = norm
    for step in range(1, n):
        left = lax.ppermute(left, "zero", [(i, i - 1) for i in range(1, n - step + 1)])
        right = lax.ppermute(right, "zero", [(i, i + 1) for i in range(step - 1, n - 1)])
        index = jnp.arange(n)[:, None]
        full = jnp.where(index == z + step, left[None], full)
        full = jnp.where(index == z - step, right[None], full)
    serve_norm = full.reshape(-1)
    return (outs[2], outs[0], outs[1], factor_query, factor_key, factor_value, serve_norm)


def sequence(n):
    query = range(2, 2 + PIECES)
    order = [(0, 1), (1, 1)]
    for step in range(1, n):
        if step + 1 < n:
            order += [(0, step + 1), (1, step + 1)]
        order += [(j, step) for j in query]
    return order


def solution(mesh):
    in_specs = (
        P(("unit", "zero"), "model"),
        P(("unit", "zero"), "model"),
        P(("unit", "zero"), "model"),
        P(("unit", "zero"), "model"),
        P(("unit", "zero"), "model"),
        P(("unit", "zero"), "model"),
        P(("unit", "zero")),
        P(("unit", "zero", "model")),
        P(("unit", "zero", "model")),
    )
    out_specs = (
        P("unit", "model"),
        P("unit", "model"),
        P("unit", "model"),
        P(("unit", "model")),
        P(("unit", "model")),
        P(("unit", "model")),
        P("unit"),
    )
    n = mesh.shape["zero"]

    def body(*args):
        return on_device(n, *args)

    return jax.shard_map(
        body, mesh=mesh, in_specs=in_specs, out_specs=out_specs, check_vma=False
    )
```
